32 devices in a mesh: groups: 2 (over y), expert: 8 (over z, core), tensor: 2 (over x).
Axes of the slice: x: 2, y: 2, z: 4, core: 2. Of those that a mesh axis runs over, the one named last changes fastest.
Arguments:
- query: bfloat16 [768, 8192], P(('groups', 'expert'), 'tensor'), parts along dimension 0, may hold values from -40 to 40
- latest_key_value: bfloat16 [768, 2, 512], P(('groups', 'expert'), None, 'tensor'), parts along dimension 0, may hold values from -6 to 6
- cache: bfloat16 [768, 2, 128, 512], P(('groups', 'expert'), None, None, 'tensor'), parts along dimension 0, may hold values from -6 to 6
- lengths: int32 [768], P(('groups', 'expert')), parts along dimension 0, may hold values from 2 to 128
- w_out: bfloat16 [8192, 4096], P('tensor', 'expert'), may hold values from -0.0625 to 0.0625
- residual_in: bfloat16 [768, 4096], P(('groups', 'expert', 'tensor')), parts along dimension 0, may hold values from -6 to 6
- norm_gain: bfloat16 [4096], replicated, may hold values from 0.5 to 1.5
- expert_ids: int32 [768, 8], P(('groups', 'expert')), parts along dimension 0, may hold values from 0 to 15, all different within a row; in each aligned block of 48 rows (0 to 47, 48 to 95, ...) at most 48 rows name the same one
- route_weights: float32 [768, 8], P(('groups', 'expert')), parts along dimension 0, may hold values from 0.05 to 0.5
- w_gate: bfloat16 [16, 4096, 768], P('expert', None, 'tensor'), may hold values from -0.09375 to 0.09375
- w_up: bfloat16 [16, 4096, 768], P('expert', None, 'tensor'), may hold values from -0.09375 to 0.09375
- w_down: bfloat16 [16, 768, 4096], P('expert', 'tensor'), may hold values from -0.21875 to 0.21875
Outputs:
- layer_out: bfloat16 [768, 4096], P(('groups', 'expert', 'tensor')), parts along dimension 0
The draws below stay inside these ranges and needn't reach their ends.
There are 2 independent parts, one for each index of `groups`. The reference program is written for one: setup_inputs(seed, part) draws one part's arguments, and reference() takes and returns one part's arrays. A program takes and returns all parts, laid end to end along the dimension named above; an argument that names none is the same for every part. Nothing has to cross between parts.
Inputs may be any that keep to these rules, and one draw needn't show every extreme that they name: `expert_ids`: the 8 entries of a row differ. Within each aligned block of 48 rows (the rows of one index of the expert axis) no expert is named by more than 48 rows, and in every draw some block reaches that bound.
All inputs are finite; a program needn't handle non-finite values.
Results may differ from the reference program's by a relative error of at most 0.0095.
Values may be sent and summed in bfloat16 or wider, within the bound.
No kernel may reach another device: no remote copies, remote signals or barrier semaphores. Data moves between devices by JAX's collectives and lax.ppermute only.
A program may use at most 128 MiB of HBM per device.

```python
import math
import jax
import jax.numpy as jnp
import numpy as np
from jax import lax

D = 4096
QUERY_HEADS = 64
KEY_VALUE_HEADS = 4
HEAD_SIZE = 128
TOP = 8
FF = 768
TOK_DEV = 48
CACHE_LENGTH = 128
EXPERTS = 16
REQUEST_TOTAL = 384
CAP = 48
N_TENSOR = 2


def cache_values(key):
    folded = jax.random.fold_in(key, 17)
    tensor_dims = (REQUEST_TOTAL, 2, CACHE_LENGTH, KEY_VALUE_HEADS * HEAD_SIZE)
    values = jnp.clip(jax.random.normal(folded, tensor_dims, jnp.float32), -6.0, 6.0)
    return values


def draw_cache(key, part):
    return cache_values(key).astype(jnp.bfloat16)


def draw_query(key, part):
    folded = jax.random.fold_in(key, 29)
    tensor_dims = (REQUEST_TOTAL, QUERY_HEADS * HEAD_SIZE)
    values = jnp.clip(jax.random.normal(folded, tensor_dims, jnp.float32), -6.0, 6.0)
    return values.astype(jnp.bfloat16)


def set_ends(result, stream_key, low, top_value):
    longest = result.shape.index(max(result.shape))
    spots = []
    for shift in (0, 1):
        where = [jax.random.randint(jax.random.fold_in(stream_key, axis), (), 0, length) for axis, length in enumerate(result.shape)]
        where[longest] = (where[longest] + shift) % result.shape[longest]
        spots.append(tuple(where))
    return result.at[spots[0]].set(low).at[spots[1]].set(top_value)


def level_of(own_key, dims, pieces, smallest, top_value):
    level = 1.0
    for axis_at, shards_of in pieces:
        draws = jax.random.uniform(jax.random.fold_in(jax.random.fold_in(own_key, 6), axis_at), (shards_of,), jnp.float32, smallest / len(pieces), top_value / len(pieces))
        level = level * jnp.repeat(jnp.exp(draws), dims[axis_at] // shards_of).reshape((-1,) + (1,) * (len(dims) - 1 - axis_at))
    return level


def routed_block(stream_key, own, number, rows, count, top, bound, slope):
    sequence = jax.random.permutation(stream_key, count)
    heavy_load, ordinary = shares(count, rows * top, bound, slope, True), shares(count, rows * top, bound, slope, False)
    places = jnp.arange(count)

    def named(sizes, turn):
        used = int((sizes > 0).sum())
        fixed = max(1, used // 4)
        shifted = fixed + (places - fixed + turn * (used - fixed)) % max(1, count - fixed)
        return jnp.zeros((count,), jnp.int32).at[sequence[jnp.where(places < fixed, places, shifted)]].set(jnp.asarray(sizes, jnp.int32))

    sizes = jnp.where(number % 4 == 0, named(heavy_load, number // 4), named(ordinary, number - number // 4 - 1))
    mixed = jax.random.permutation(jax.random.fold_in(own, 3), count)
    donor, taker = mixed[0:count // 2 * 2:2], mixed[1:count // 2 * 2:2]
    slack = jnp.minimum(sizes[donor] - 1, bound - sizes[taker]) // 2
    slack = jnp.where((donor == sequence[0]) | (taker == sequence[0]) | (sizes[taker] == 0), 0, jnp.maximum(slack, 0))
    shifted = jax.random.randint(jax.random.fold_in(own, 4), (count // 2,), 0, 1 << 20) % (slack + 1)
    sizes = sizes.at[donor].add(-shifted).at[taker].add(shifted)
    items = jnp.searchsorted(jnp.cumsum(sizes), jnp.arange(rows * top), side="right").astype(jnp.int32)
    table = items.reshape(top, rows).T
    table = table[jax.random.permutation(jax.random.fold_in(own, 1), rows)]
    turn = jax.random.randint(jax.random.fold_in(own, 2), (rows, 1), 0, top)
    return jnp.take_along_axis(table, (jnp.arange(top)[None, :] + turn) % top, axis=1)


def shares(count, total, most, slope, full):
    weights = [(1 << 20) // math.isqrt(rank ** slope) + 1 for rank in range(1, count + 1)]
    largest = most if full else min(most, max(-(-total // count), total * weights[0] // sum(weights)))
    least = 1 if total - largest >= count - 1 else 0
    counts, spare = [largest] + [least] * (count - 1), total - largest - least * (count - 1)
    while spare > 0:
        movable = [i for i in range(1, count) if counts[i] < largest] or [i for i in range(1, count) if counts[i] < most]
        whole, budget = sum([weights[i] for i in movable]), spare
        for i in movable:
            more = min(most - counts[i], max(1, budget * weights[i] // whole), spare)
            counts[i] = counts[i] + more
            spare = spare - more
    return np.array(counts)


def centred(stream_key, dims, width, bound, cuts=(), held_as=jnp.bfloat16):
    values = width * jax.random.normal(stream_key, dims, jnp.float32)
    if cuts:
        values = values * level_of(stream_key, dims, cuts, -0.22, 0.18)
    return jnp.clip(values, -bound, bound).astype(held_as)


def setup_inputs(seed: int = 0, part: int = 0) -> dict:
    splits = jax.random.split(jax.random.key(seed), 13)
    part_splits = jax.random.split(jax.random.fold_in(splits[12], part), 13)
    query = draw_query(jax.random.fold_in(jax.random.fold_in(splits[12], part), 71), part)
    latest_key_value = centred(part_splits[1], (REQUEST_TOTAL, 2, KEY_VALUE_HEADS * HEAD_SIZE), 1.0, 6.0, ((0, 8), (2, 2)))
    cache = draw_cache(jax.random.fold_in(jax.random.fold_in(splits[12], part), 71), part)
    lengths = set_ends(jax.random.randint(part_splits[3], (REQUEST_TOTAL,), 2, CACHE_LENGTH + 1), jax.random.fold_in(part_splits[3], 1), 2, CACHE_LENGTH).astype(jnp.int32)
    w_out = centred(splits[4], (QUERY_HEADS * HEAD_SIZE, D), (QUERY_HEADS * HEAD_SIZE) ** -0.5, 0.0625, ((0, 2), (1, 8)))
    residual_in = centred(part_splits[5], (REQUEST_TOTAL, D), 1.0, 6.0, ((0, 16),))
    norm_gain = jnp.clip(1.0 + 0.1 * jax.random.normal(splits[6], (D,), jnp.float32), 0.5, 1.5).astype(jnp.bfloat16)
    expert_ids_keys = jax.random.split(jax.random.fold_in(part_splits[7], 1), REQUEST_TOTAL // TOK_DEV)
    expert_ids_turns = jax.random.permutation(jax.random.fold_in(part_splits[7], 3), REQUEST_TOTAL // TOK_DEV)
    expert_ids = jax.vmap(lambda own, number: routed_block(jax.random.fold_in(part_splits[7], 2), own, number, TOK_DEV, EXPERTS, TOP, CAP, 2))(expert_ids_keys, expert_ids_turns).reshape((REQUEST_TOTAL, TOP))
    route_weights = jnp.clip(jnp.exp(math.log(0.5) - 2.3025851 * jax.random.uniform(part_splits[8], (REQUEST_TOTAL, TOP), jnp.float32) ** level_of(part_splits[8], (REQUEST_TOTAL, TOP), ((0, 8),), -0.2, 0.2)), 0.05, 0.5)
    w_gate = centred(splits[9], (EXPERTS, D, FF), D ** -0.5, 0.09375, ((0, 8), (2, 2)))
    w_up = centred(splits[10], (EXPERTS, D, FF), D ** -0.5, 0.09375, ((0, 8), (2, 2)))
    w_down = centred(splits[11], (EXPERTS, FF, D), FF ** -0.5, 0.21875, ((0, 8), (1, 2)))
    return {"query": query, "latest_key_value": latest_key_value, "cache": cache, "lengths": lengths, "w_out": w_out, "residual_in": residual_in, "norm_gain": norm_gain, "expert_ids": expert_ids, "route_weights": route_weights, "w_gate": w_gate, "w_up": w_up, "w_down": w_down}


block_rows = 64

def attention(query, latest_key_value, cache, lengths):
    token_count = query.shape[0]
    kv_heads = latest_key_value.shape[2] // HEAD_SIZE
    group_size = query.shape[1] // (kv_heads * HEAD_SIZE)
    positions = cache.shape[2]
    factor = 1.0 / math.sqrt(HEAD_SIZE)
    queries = query.astype(jnp.float32).reshape(token_count, kv_heads, group_size, HEAD_SIZE)
    cached_keys = cache[:, 0].astype(jnp.float32).reshape(token_count, positions, kv_heads, HEAD_SIZE)
    cached_values = cache[:, 1].astype(jnp.float32).reshape(token_count, positions, kv_heads, HEAD_SIZE)
    fresh_keys = latest_key_value[:, 0].astype(jnp.float32).reshape(token_count, kv_heads, HEAD_SIZE)
    fresh_values = latest_key_value[:, 1].astype(jnp.float32).reshape(token_count, kv_heads, HEAD_SIZE)
    scores = jnp.einsum('tkgd,tlkd->tkgl', queries, cached_keys) * factor
    valid = jnp.arange(positions, dtype=jnp.int32)[None, :] < lengths[:, None]
    scores = jnp.where(valid[:, None, None, :], scores, -jnp.inf)
    own_score = jnp.einsum('tkgd,tkd->tkg', queries, fresh_keys) * factor
    highest = jnp.maximum(lax.optimization_barrier(jnp.max(scores, axis=-1)), own_score)
    weights = jnp.exp(scores - highest[..., None])
    own_weight = jnp.exp(own_score - highest)
    total = lax.optimization_barrier(jnp.sum(weights, axis=-1)) + own_weight
    probs = lax.optimization_barrier((weights / total[..., None]).astype(jnp.bfloat16))
    own_prob = lax.optimization_barrier((own_weight / total).astype(jnp.bfloat16))
    mixed = jnp.einsum('tkgl,tlkd->tkgd', probs.astype(jnp.float32), cached_values)
    mixed = mixed + own_prob.astype(jnp.float32)[..., None] * fresh_values[:, :, None, :]
    return mixed.reshape(token_count, -1).astype(jnp.bfloat16)

def reference(query, latest_key_value, cache, lengths, w_out, residual_in, norm_gain, expert_ids, route_weights, w_gate, w_up, w_down):
    attended = attention(query, latest_key_value, cache, lengths)
    stream = residual_in.astype(jnp.float32) + jnp.dot(attended, w_out, preferred_element_type=jnp.float32)
    meansq = lax.optimization_barrier(jnp.mean(stream * stream, axis=-1, keepdims=True))
    normed = (stream * lax.rsqrt(meansq + 1e-06) * norm_gain.astype(jnp.float32)).astype(jnp.bfloat16)
    assignments = REQUEST_TOTAL * TOP
    flat_ids = expert_ids.reshape(-1).astype(jnp.int32)
    sort_order = jnp.argsort(flat_ids, stable=True).astype(jnp.int32)
    sorted_ids = flat_ids[sort_order]
    expert_counts = lax.optimization_barrier(jnp.sum((flat_ids[:, None] == jnp.arange(EXPERTS, dtype=jnp.int32)[None, :]).astype(jnp.int32), axis=0))
    first_index = jnp.cumsum(expert_counts) - expert_counts
    rank_within = jnp.arange(assignments, dtype=jnp.int32) - first_index[sorted_ids]
    padded_counts = (expert_counts + block_rows - 1) // block_rows * block_rows
    padded_start = jnp.cumsum(padded_counts) - padded_counts
    position_sorted = (padded_start[sorted_ids] + rank_within).astype(jnp.int32)
    block_count = (assignments + block_rows - 1) // block_rows + EXPERTS
    position_of = jnp.zeros((assignments,), jnp.int32).at[sort_order].set(position_sorted)
    slot_token = jnp.zeros((block_count * block_rows,), jnp.int32).at[position_sorted].set(sort_order // TOP)
    block_starts = jnp.arange(block_count, dtype=jnp.int32) * block_rows
    block_expert = lax.optimization_barrier(jnp.sum((padded_start[None, :] <= block_starts[:, None]).astype(jnp.int32), axis=1)) - 1
    block_expert = jnp.clip(block_expert, 0, EXPERTS - 1).astype(jnp.int32)
    width_part = FF // N_TENSOR

    def run_block(block_index):
        chosen = block_expert[block_index]
        token_index = lax.dynamic_slice_in_dim(slot_token, block_index * block_rows, block_rows)
        inputs = normed[token_index]
        gate_proj = jnp.dot(inputs, w_gate[chosen], preferred_element_type=jnp.float32)
        up_proj = jnp.dot(inputs, w_up[chosen], preferred_element_type=jnp.float32)
        activated = (jax.nn.silu(gate_proj) * up_proj).astype(jnp.bfloat16)
        down_rows = w_down[chosen]
        summed = jnp.zeros((block_rows, D), jnp.float32)
        for piece in range(N_TENSOR):
            term = jnp.dot(activated[:, piece * width_part:(piece + 1) * width_part], down_rows[piece * width_part:(piece + 1) * width_part], preferred_element_type=jnp.float32)
            rounded = lax.optimization_barrier(term.astype(jnp.bfloat16))
            summed = summed + rounded.astype(jnp.float32)
        return summed.astype(jnp.bfloat16)
    outputs = lax.map(run_block, jnp.arange(block_count, dtype=jnp.int32)).reshape(block_count * block_rows, D)
    per_choice = outputs[position_of].astype(jnp.float32).reshape(REQUEST_TOTAL, TOP, D)
    mixture = lax.optimization_barrier(jnp.sum(route_weights.astype(jnp.float32)[:, :, None] * per_choice, axis=1))
    return (stream + mixture).astype(jnp.bfloat16)
```

```python
import functools
import math

import jax
import jax.numpy as jnp
from jax import lax
from jax.experimental import pallas as pl
from jax.experimental.pallas import tpu as pltpu
from jax.sharding import PartitionSpec as P

HEAD_SIZE = 128
CORES = 2
BF16 = jnp.bfloat16
F32 = jnp.float32


NT = (((1,), (1,)), ((), ()))


def fold_order(count):
    return list(range(0, count, 2)) + list(range(count - 1 - count % 2, 0, -2))


def chip_perm(chips, shift):
    order = fold_order(chips)
    place = {z: i for i, z in enumerate(order)}
    to = lambda z: order[(place[z] + shift) % chips]
    return [(z * CORES + c, to(z) * CORES + c) for z in range(chips) for c in range(CORES)]


def core_perm(chips):
    return [(z * CORES + c, z * CORES + 1 - c) for z in range(chips) for c in range(CORES)]


def chip_table(chips, sign):
    order = fold_order(chips)
    place = {z: i for i, z in enumerate(order)}
    return [[order[(place[z] + sign * s) % chips] for s in range(chips)] for z in range(chips)]


def chip_send(piece, chips, shift):
    return lax.ppermute(piece, "expert", chip_perm(chips, shift))


def core_swap(piece, chips):
    return lax.ppermute(piece, "expert", core_perm(chips))


def tensor_shift(piece, tensors, shift):
    return lax.ppermute(piece, "tensor", [((i + shift) % tensors, i) for i in range(tensors)])


def chip_gather(piece, chips):
    pieces = [None] * chips
    pieces[0] = piece
    ahead = back = piece
    for s in range(1, chips // 2 + 1):
        if pieces[s] is None:
            ahead = chip_send(ahead, chips, 1)
            pieces[s] = ahead
        if pieces[chips - s] is None:
            back = chip_send(back, chips, -1)
            pieces[chips - s] = back
    return pieces


def chip_scatter(take, chips):
    total = take(0)
    for sign, steps in ((1, chips // 2), (-1, (chips - 1) // 2)):
        held = None
        for s in range(steps, 0, -1):
            own = take(s if sign > 0 else chips - s)
            held = own if held is None else own + held
            held = chip_send(held.astype(BF16), chips, sign)
            held = held.astype(F32)
        if held is not None:
            total = total + held
    return total


def attention_kernel(
    chunk, kv_heads, head_count, tab_ref, len_ref, q_ref, new_ref, cache_ref, out_ref, qs, buf, sems
):
    rows = q_ref.shape[1]
    group = head_count // kv_heads
    factor = 1.0 / math.sqrt(HEAD_SIZE)
    first = tab_ref[0] * rows
    pitch = qs.shape[0] // rows

    copies = []
    for c in range(rows // chunk):
        copies.append(
            pltpu.make_async_copy(
                cache_ref.at[pl.ds(first + c * chunk, chunk)],
                buf.at[pl.ds(c * chunk, chunk)],
                sems.at[c],
            )
        )
        copies[-1].start()
    for h in range(head_count):
        qs[pl.ds(h, rows, stride=pitch), :] = q_ref[
            0, :, h * HEAD_SIZE : (h + 1) * HEAD_SIZE
        ].astype(F32)

    positions = buf.shape[2]
    block = chunk * head_count
    pos = lax.broadcasted_iota(jnp.int32, (head_count, positions), 1)
    head_kv = lax.broadcasted_iota(jnp.int32, (block, HEAD_SIZE), 0) // group % kv_heads
    wide = (head_count, new_ref.shape[3])
    for c in range(rows // chunk):
        span = range(c * chunk, (c + 1) * chunk)
        q32 = jnp.concatenate([qs[t * pitch : t * pitch + head_count, :] for t in span], axis=0)
        spread = [jnp.where(head_kv == kv, q32, 0.0) for kv in range(kv_heads)]
        q = spread[0] if kv_heads == 1 else jnp.concatenate(spread, axis=1)
        q16 = q.astype(BF16)
        keys = [jnp.broadcast_to(new_ref[0, t, 0:1, :].astype(F32), wide) for t in span]
        values = [jnp.broadcast_to(new_ref[0, t, 1:2, :].astype(F32), wide) for t in span]
        own = jnp.sum(q * jnp.concatenate(keys, axis=0), axis=1, keepdims=True) * factor
        copies[c].wait()
        scores = []
        for i, t in enumerate(span):
            score = lax.dot_general(
                q16[i * head_count : (i + 1) * head_count],
                buf[t, 0],
                NT,
                preferred_element_type=F32,
            )
            scores.append(jnp.where(pos < len_ref[first + t], score * factor, -jnp.inf))
        scores = jnp.concatenate(scores, axis=0)
        highest = jnp.maximum(jnp.max(scores, axis=1, keepdims=True), own)
        weights = jnp.exp(scores - highest)
        own_weight = jnp.exp(own - highest)
        inverse = 1.0 / (jnp.sum(weights, axis=1, keepdims=True) + own_weight)
        probs = (weights * inverse).astype(BF16)
        own_prob = (own_weight * inverse).astype(BF16).astype(F32)
        mixed = jnp.concatenate(
            [
                jnp.dot(
                    probs[i * head_count : (i + 1) * head_count],
                    buf[t, 1],
                    preferred_element_type=F32,
                )
                for i, t in enumerate(span)
            ],
            axis=0,
        )
        mixed = mixed + own_prob * jnp.concatenate(values, axis=0)
        out = mixed[:, :HEAD_SIZE]
        for kv in range(1, kv_heads):
            out = jnp.where(head_kv == kv, mixed[:, kv * HEAD_SIZE : (kv + 1) * HEAD_SIZE], out)
        for i, t in enumerate(span):
            qs[t * pitch : t * pitch + head_count, :] = out[i * head_count : (i + 1) * head_count]

    for h in range(head_count):
        out_ref[:, h * HEAD_SIZE : (h + 1) * HEAD_SIZE] = qs[
            pl.ds(h, rows, stride=pitch), :
        ].astype(BF16)


def attend(part, query, latest, cache, lengths, parts):
    token_count, width = query.shape
    rows = token_count // parts
    kv_width = latest.shape[2]
    kv_heads = kv_width // HEAD_SIZE
    head_count = width // HEAD_SIZE
    chunk = next(k for k in (8, 6, 4, 3, 2, 1) if rows % k == 0)
    return pl.pallas_call(
        functools.partial(attention_kernel, chunk, kv_heads, head_count),
        grid_spec=pltpu.PrefetchScalarGridSpec(
            num_scalar_prefetch=2,
            grid=(1,),
            in_specs=[
                pl.BlockSpec((1, rows, width), lambda i, tab, ln: (tab[0], 0, 0)),
                pl.BlockSpec((1, rows, 2, kv_width), lambda i, tab, ln: (tab[0], 0, 0, 0)),
                pl.BlockSpec(memory_space=pltpu.HBM),
            ],
            out_specs=pl.BlockSpec((rows, width), lambda i, tab, ln: (0, 0)),
            scratch_shapes=[
                pltpu.VMEM((rows * (head_count + 8), HEAD_SIZE), F32),
                pltpu.VMEM((rows,) + cache.shape[1:], BF16),
                pltpu.SemaphoreType.DMA((rows // chunk,)),
            ],
        ),
        out_shape=jax.ShapeDtypeStruct((rows, width), BF16),
        compiler_params=pltpu.CompilerParams(
            dimension_semantics=("arbitrary",), vmem_limit_bytes=12 << 20
        ),
        name="attend",
    )(
        part.reshape(1),
        lengths,
        *in_hbm(
            query.reshape(parts, rows, width), latest.reshape(parts, rows, 2, kv_width), cache
        ),
    )


def in_hbm(*arrays):
    return [pltpu.with_memory_space_constraint(a, pltpu.HBM) for a in arrays]


def project_kernel(count, steps, tab_ref, *refs):
    pieces, w_ref, adds, out_ref, buf, sems = (
        refs[:count],
        refs[count],
        refs[count + 1 : -3],
        refs[-3],
        refs[-2],
        refs[-1],
    )
    rows, width = pieces[0].shape
    columns = w_ref.shape[1]
    deep = width // steps
    copies = [
        pltpu.make_async_copy(
            w_ref.at[pl.ds(k * deep, deep)], buf.at[pl.ds(k * deep, deep)], sems.at[k]
        )
        for k in range(steps)
    ]
    for copy in copies:
        copy.start()
    result = None
    for k in range(steps):
        span = slice(k * deep, (k + 1) * deep)
        lhs = jnp.concatenate([p[:, span].astype(F32) for p in pieces], axis=0).astype(BF16)
        copies[k].wait()
        term = jnp.dot(lhs, buf[span, :], preferred_element_type=F32)
        result = term if result is None else result + term
    for i in range(count):
        block = tab_ref[i]
        value = result[i * rows : (i + 1) * rows]
        for a in adds:
            value = value + a[block][:, :columns].astype(F32)
        out_ref[block] = value.astype(BF16)


def project(table, pieces, w_out, adds):
    rows, _ = pieces[0].shape
    count = len(pieces)
    steps = 4
    vmem = pl.BlockSpec(memory_space=pltpu.VMEM)
    hbm = pl.BlockSpec(memory_space=pltpu.HBM)
    return pl.pallas_call(
        functools.partial(project_kernel, count, steps),
        in_specs=[pl.BlockSpec(memory_space=pltpu.SMEM)]
        + [vmem] * count
        + [hbm]
        + [vmem] * len(adds),
        out_specs=vmem,
        out_shape=jax.ShapeDtypeStruct((count, rows, w_out.shape[1]), BF16),
        scratch_shapes=[
            pltpu.VMEM(w_out.shape, BF16),
            pltpu.SemaphoreType.DMA((steps,)),
        ],
        compiler_params=pltpu.CompilerParams(vmem_limit_bytes=16 << 20),
        name="project",
    )(table, *pieces, *in_hbm(w_out), *adds)


def load_down(wd_ref, wd_buf, sem, first):
    columns = wd_buf.shape[2]
    return pltpu.make_async_copy(wd_ref.at[:, :, pl.ds(first, columns)], wd_buf, sem)


def down_product(acts, wd_buf, tab_ref, send_ref, keep_ref):
    local, hidden, columns = wd_buf.shape
    chips = acts[0].shape[1]
    count = chips * CORES
    core = tab_ref[count + 1]
    block = min(columns, 1024)
    aligned = hidden % 128 == 0
    for out_ref, half in ((send_ref, 1 - core), (keep_ref, core)):
        lhs = []
        for e in range(local):
            picked = [
                act[e, tab_ref[count + 2 + s], half].astype(F32)
                for act in acts
                for s in range(chips)
            ]
            lhs.append(jnp.concatenate(picked, axis=0).astype(BF16))
        if aligned:
            lhs = [jnp.concatenate(lhs, axis=1)]
        for b in range(columns // block):
            span = slice(b * block, (b + 1) * block)
            if aligned:
                right = [wd_buf[:, :, span].reshape(local * hidden, block)]
            else:
                right = [wd_buf[e, :, span] for e in range(local)]
            result = sum(jnp.dot(l, r, preferred_element_type=F32) for l, r in zip(lhs, right))
            out_ref[:, :, :, span] = result.astype(BF16).reshape(out_ref.shape[:3] + (block,))


def up_kernel(part, last, count, tab_ref, *refs):
    refs = list(refs)
    slices = [refs.pop(0) for _ in range(count)]
    gain_ref, weight_ref, wg_ref, wu_ref = [refs.pop(0) for _ in range(4)]
    acts = [refs.pop(0) for _ in range(part)] if last else []
    wd_ref = refs.pop(0) if last else None
    act_ref = refs.pop(0)
    own_ref = refs.pop(0) if part == 0 else None
    send_ref, keep_ref = (refs.pop(0), refs.pop(0)) if last else (None, None)
    wg_buf, wu_buf, sems = [refs.pop(0) for _ in range(3)]
    local, features, hidden = wg_ref.shape
    _, rows, columns = slices[0].shape
    total = count * rows
    aligned = hidden % 128 == 0

    def span_of(i):
        return pl.ds(pl.multiple_of(tab_ref[i] * columns, columns), columns)

    copies = [
        [
            pltpu.make_async_copy(src.at[:, span_of(i), :], dst.at[:, span_of(i), :], sems.at[k, i])
            for k, (src, dst) in enumerate(((wg_ref, wg_buf), (wu_ref, wu_buf)))
        ]
        for i in range(count)
    ]
    for pair in copies:
        for copy in pair:
            copy.start()
    if last:
        down = load_down(wd_ref, refs[0], refs[1].at[0], 0)
        down.start()
    squares = jnp.zeros((total, 1), F32)
    sums = None
    for i in range(count):
        span = span_of(i)
        if part == 0:
            own_ref[:, span] = slices[i][tab_ref[count]]
        x = slices[i][...].astype(F32).reshape(total, columns)
        squares = squares + jnp.sum(x * x, axis=1, keepdims=True)
        scaled = (x * gain_ref[:, span].astype(F32)).astype(BF16)
        for copy in copies[i]:
            copy.wait()
        weights = [w[e, span, :] for w in (wg_buf, wu_buf) for e in range(local)]
        if aligned:
            weights = [jnp.concatenate(weights, axis=1)]
        more = [jnp.dot(scaled, w, preferred_element_type=F32) for w in weights]
        sums = more if sums is None else [a + b for a, b in zip(sums, more)]
    if aligned:
        sums = [sums[0][:, k * hidden : (k + 1) * hidden] for k in range(2 * local)]
    scale = lax.rsqrt(squares * (1.0 / features) + 1e-06)
    for e in range(local):
        gate = sums[e] * scale
        up = sums[local + e] * scale
        chosen = weight_ref[part, :, e : e + 1]
        value = gate / (1.0 + jnp.exp(-gate)) * up * chosen
        value = jnp.where(chosen != 0.0, value, 0.0).astype(BF16)
        for i in range(count):
            act_ref[e, i // CORES, i % CORES] = value[i * rows : (i + 1) * rows]
    if last:
        down.wait()
        down_product(acts + [act_ref], refs[0], tab_ref, send_ref, keep_ref)


def expert_up(table, part, slices, gain, weights, w_gate, w_up, acts=None, w_down=None, pieces=1):
    count = len(slices)
    local, features, hidden = w_gate.shape
    _, rows, _ = slices[0].shape
    chips = count // CORES
    vmem = pl.BlockSpec(memory_space=pltpu.VMEM)
    hbm = pl.BlockSpec(memory_space=pltpu.HBM)
    last = w_down is not None
    shapes = [jax.ShapeDtypeStruct((local, chips, CORES, rows, hidden), BF16)]
    if part == 0:
        shapes.append(jax.ShapeDtypeStruct((rows, features), BF16))
    specs = [pl.BlockSpec(memory_space=pltpu.SMEM)] + [vmem] * (count + 2) + [hbm] * 2
    operands = [table, *slices, gain.reshape(1, -1), weights, *in_hbm(w_gate, w_up)]
    scratch = [
        pltpu.VMEM(w_gate.shape, BF16),
        pltpu.VMEM(w_up.shape, BF16),
        pltpu.SemaphoreType.DMA((2, count)),
    ]
    if last:
        wide = features // pieces
        shapes += [jax.ShapeDtypeStruct((part + 1, chips, rows, wide), BF16)] * 2
        specs += [vmem] * part + [hbm]
        operands += [*acts, *in_hbm(w_down)]
        scratch += [pltpu.VMEM((local, hidden, wide), BF16), pltpu.SemaphoreType.DMA((1,))]
    return pl.pallas_call(
        functools.partial(up_kernel, part, last, count),
        in_specs=specs,
        out_specs=[vmem] * len(shapes),
        out_shape=shapes,
        scratch_shapes=scratch,
        compiler_params=pltpu.CompilerParams(vmem_limit_bytes=(34 if last else 26) << 20),
        name="expert_up",
    )(*operands)


def down_kernel(tensors, first, tab_ref, *refs):
    acts, (wd_ref, send_ref, keep_ref, wd_buf, sem) = refs[:tensors], refs[tensors:]
    copy = load_down(wd_ref, wd_buf, sem.at[0], first)
    copy.start()
    copy.wait()
    down_product(acts, wd_buf, tab_ref, send_ref, keep_ref)


def expert_down(table, acts, w_down, piece, pieces):
    local, chips, _, rows, hidden = acts[0].shape
    columns = w_down.shape[2] // pieces
    vmem = pl.BlockSpec(memory_space=pltpu.VMEM)
    half = jax.ShapeDtypeStruct((len(acts), chips, rows, columns), BF16)
    return pl.pallas_call(
        functools.partial(down_kernel, len(acts), piece * columns),
        in_specs=[pl.BlockSpec(memory_space=pltpu.SMEM)]
        + [vmem] * len(acts)
        + [pl.BlockSpec(memory_space=pltpu.HBM)],
        out_specs=[vmem] * 2,
        out_shape=[half, half],
        scratch_shapes=[
            pltpu.VMEM((local, hidden, columns), BF16),
            pltpu.SemaphoreType.DMA((1,)),
        ],
        compiler_params=pltpu.CompilerParams(vmem_limit_bytes=20 << 20),
        name="expert_down",
    )(table, *acts, *in_hbm(w_down))


def per_device(
    query,
    latest_key_value,
    cache,
    lengths,
    w_out,
    residual_in,
    norm_gain,
    expert_ids,
    route_weights,
    w_gate,
    w_up,
    w_down,
):
    count = lax.axis_size("expert")
    tensors = lax.axis_size("tensor")
    chips = count // CORES
    me = lax.axis_index("expert")
    mine = lax.axis_index("tensor")
    core = me % CORES
    chip = me // CORES
    token_count = query.shape[0]
    rows = token_count // tensors
    columns = w_out.shape[1]
    local = w_gate.shape[0]
    features = residual_in.shape[1]

    behind = jnp.take(jnp.array(chip_table(chips, -1), jnp.int32), chip, axis=0)
    ahead = jnp.take(jnp.array(chip_table(chips, 1), jnp.int32), chip, axis=0)
    blocks = jnp.concatenate([behind * CORES + core, behind * CORES + (1 - core)])
    table = jnp.concatenate([blocks, me[None], core[None], ahead]).astype(jnp.int32)

    named = expert_ids[:, :, None] == jnp.arange(local * count, dtype=jnp.int32)
    dense = jnp.sum(jnp.where(named, route_weights[:, :, None], 0.0), axis=1)
    high = dense.astype(BF16)
    low = (dense - high.astype(F32)).astype(BF16)
    pair = jnp.stack([high, low], axis=-1).reshape(tensors, rows, count, local * 2)
    pair = jnp.roll(pair, -mine, axis=0)
    pair = pair.transpose(2, 1, 0, 3).reshape(count, rows, tensors * local * 2)
    pair = jnp.pad(pair, ((0, 0), (0, 0), (0, 128 - pair.shape[2])))
    shares = residual_in.reshape(rows, count, columns).transpose(1, 0, 2)
    packed = jnp.concatenate([shares, pair], axis=2)
    given = lax.all_to_all(packed, "expert", split_axis=0, concat_axis=0, tiled=True)
    pair = given[:, :, columns : columns + tensors * local * 2].astype(F32)
    pair = pair.reshape(count, rows, tensors, local, 2).sum(axis=-1)
    weights = pair.transpose(2, 0, 1, 3).reshape(tensors, count * rows, local)

    passed = []
    for j in range(1, tensors + 1):
        part = (mine + j) % tensors
        attended = attend(part, query, latest_key_value, cache, lengths, tensors)
        pieces = chip_gather(attended, chips)
        pieces = pieces + [core_swap(p, chips) for p in pieces]
        adds = [] if j < tensors else passed + [given]
        stream = project(table, pieces, w_out, adds)
        if j < tensors:
            passed.append(tensor_shift(stream, tensors, -j))

    gathered = chip_gather(stream, chips)
    acts = []
    for j in range(tensors):
        held = gathered
        if j:
            held = [tensor_shift(p, tensors, j) for p in gathered]
        held = held + [core_swap(p, chips) for p in held]
        rest = (acts, w_down, 2) if j == tensors - 1 else ()
        act, *more = expert_up(table, j, held, norm_gain, weights, w_gate, w_up, *rest)
        acts.append(act)
        if j == 0:
            mine_rows = more.pop(0)

    half = features // 2
    sums = []
    for part in range(2):
        if part:
            more = expert_down(table, acts, w_down, part, 2)
        send, keep = more
        both = keep.astype(F32) + core_swap(send, chips).astype(F32)
        for axis in (("t", "z") if part == 0 else ("z", "t")):
            if axis == "t":
                kept = both[0]
                for j in range(1, tensors):
                    moved = tensor_shift(both[j].astype(BF16), tensors, -j)
                    kept = kept + moved.astype(F32)
                both = kept[None]
            else:
                both = chip_scatter(lambda s, both=both: both[:, s], chips)[:, None]
        sums.append(both.reshape(rows, half))
    return (mine_rows.astype(F32) + jnp.concatenate(sums, axis=1)).astype(BF16)


def solution(mesh):
    placed = (
        P(("groups", "expert"), "tensor"),
        P(("groups", "expert"), None, "tensor"),
        P(("groups", "expert"), None, None, "tensor"),
        P(("groups", "expert")),
        P("tensor", "expert"),
        P(("groups", "expert", "tensor"), None),
        P(),
        P(("groups", "expert"), None),
        P(("groups", "expert"), None),
        P("expert", None, "tensor"),
        P("expert", None, "tensor"),
        P("expert", "tensor", None),
    )

    return jax.shard_map(
        per_device,
        mesh=mesh,
        in_specs=placed,
        out_specs=P(("groups", "expert", "tensor"), None),
        check_vma=False,
    )
```

```python
import functools
import math

import jax
import jax.numpy as jnp
from jax import lax
from jax.experimental import pallas as pl
from jax.experimental.pallas import tpu as pltpu
from jax.sharding import PartitionSpec as P

HEAD_SIZE = 128
CORES = 2
BF16 = jnp.bfloat16
F32 = jnp.float32


NT = (((1,), (1,)), ((), ()))


def fold_order(count):
    return list(range(0, count, 2)) + list(range(count - 1 - count % 2, 0, -2))


def chip_perm(chips, shift):
    order = fold_order(chips)
    place = {z: i for i, z in enumerate(order)}
    to = lambda z: order[(place[z] + shift) % chips]
    return [(z * CORES + c, to(z) * CORES + c) for z in range(chips) for c in range(CORES)]


def core_perm(chips):
    return [(z * CORES + c, z * CORES + 1 - c) for z in range(chips) for c in range(CORES)]


def chip_table(chips, sign):
    order = fold_order(chips)
    place = {z: i for i, z in enumerate(order)}
    return [[order[(place[z] + sign * s) % chips] for s in range(chips)] for z in range(chips)]


def chip_send(piece, chips, shift):
    return lax.ppermute(piece, "expert", chip_perm(chips, shift))


def core_swap(piece, chips):
    return lax.ppermute(piece, "expert", core_perm(chips))


def tensor_shift(piece, tensors, shift):
    return lax.ppermute(piece, "tensor", [((i + shift) % tensors, i) for i in range(tensors)])


def chip_gather(piece, chips):
    pieces = [None] * chips
    pieces[0] = piece
    ahead = back = piece
    for s in range(1, chips // 2 + 1):
        if pieces[s] is None:
            ahead = chip_send(ahead, chips, 1)
            pieces[s] = ahead
        if pieces[chips - s] is None:
            back = chip_send(back, chips, -1)
            pieces[chips - s] = back
    return pieces


def chip_scatter(pieces, chips):
    arrived = []
    for sign, steps in ((1, chips // 2), (-1, (chips - 1) // 2)):
        held = None
        for s in range(steps, 0, -1):
            own = pieces[s if sign > 0 else chips - s]
            held = own if held is None else add(own, held)
            held = chip_send(held, chips, sign)
        if held is not None:
            arrived.append(held)
    return arrived


def attention_kernel(
    chunk, kv_heads, head_count, tab_ref, len_ref, q_ref, new_ref, cache_ref, out_ref, qs, buf, sems
):
    rows = q_ref.shape[1]
    group = head_count // kv_heads
    factor = 1.0 / math.sqrt(HEAD_SIZE)
    first = tab_ref[0] * rows
    pitch = qs.shape[0] // rows

    copies = []
    for c in range(rows // chunk):
        copies.append(
            pltpu.make_async_copy(
                cache_ref.at[pl.ds(first + c * chunk, chunk)],
                buf.at[pl.ds(c * chunk, chunk)],
                sems.at[c],
            )
        )
        copies[-1].start()
    for h in range(head_count):
        qs[pl.ds(h, rows, stride=pitch), :] = q_ref[
            0, :, h * HEAD_SIZE : (h + 1) * HEAD_SIZE
        ].astype(F32)

    positions = buf.shape[2]
    block = chunk * head_count
    pos = lax.broadcasted_iota(jnp.int32, (head_count, positions), 1)
    head_kv = lax.broadcasted_iota(jnp.int32, (block, HEAD_SIZE), 0) // group % kv_heads
    wide = (head_count, new_ref.shape[3])
    for c in range(rows // chunk):
        span = range(c * chunk, (c + 1) * chunk)
        q32 = jnp.concatenate([qs[t * pitch : t * pitch + head_count, :] for t in span], axis=0)
        spread = [jnp.where(head_kv == kv, q32, 0.0) for kv in range(kv_heads)]
        q = spread[0] if kv_heads == 1 else jnp.concatenate(spread, axis=1)
        q16 = q.astype(BF16)
        keys = [jnp.broadcast_to(new_ref[0, t, 0:1, :].astype(F32), wide) for t in span]
        values = [jnp.broadcast_to(new_ref[0, t, 1:2, :].astype(F32), wide) for t in span]
        own = jnp.sum(q * jnp.concatenate(keys, axis=0), axis=1, keepdims=True) * factor
        copies[c].wait()
        scores = []
        for i, t in enumerate(span):
            score = lax.dot_general(
                q16[i * head_count : (i + 1) * head_count],
                buf[t, 0],
                NT,
                preferred_element_type=F32,
            )
            scores.append(jnp.where(pos < len_ref[first + t], score * factor, -jnp.inf))
        scores = jnp.concatenate(scores, axis=0)
        highest = jnp.maximum(jnp.max(scores, axis=1, keepdims=True), own)
        weights = jnp.exp(scores - highest)
        own_weight = jnp.exp(own - highest)
        inverse = 1.0 / (jnp.sum(weights, axis=1, keepdims=True) + own_weight)
        probs = (weights * inverse).astype(BF16)
        own_prob = (own_weight * inverse).astype(BF16).astype(F32)
        mixed = jnp.concatenate(
            [
                jnp.dot(
                    probs[i * head_count : (i + 1) * head_count],
                    buf[t, 1],
                    preferred_element_type=F32,
                )
                for i, t in enumerate(span)
            ],
            axis=0,
        )
        mixed = mixed + own_prob * jnp.concatenate(values, axis=0)
        out = mixed[:, :HEAD_SIZE]
        for kv in range(1, kv_heads):
            out = jnp.where(head_kv == kv, mixed[:, kv * HEAD_SIZE : (kv + 1) * HEAD_SIZE], out)
        for i, t in enumerate(span):
            qs[t * pitch : t * pitch + head_count, :] = out[i * head_count : (i + 1) * head_count]

    for h in range(head_count):
        out_ref[:, h * HEAD_SIZE : (h + 1) * HEAD_SIZE] = qs[
            pl.ds(h, rows, stride=pitch), :
        ].astype(BF16)


def attend(part, query, latest, cache, lengths, parts):
    token_count, width = query.shape
    rows = token_count // parts
    kv_width = latest.shape[2]
    kv_heads = kv_width // HEAD_SIZE
    head_count = width // HEAD_SIZE
    chunk = next(k for k in (8, 6, 4, 3, 2, 1) if rows % k == 0)
    return pl.pallas_call(
        functools.partial(attention_kernel, chunk, kv_heads, head_count),
        grid_spec=pltpu.PrefetchScalarGridSpec(
            num_scalar_prefetch=2,
            grid=(1,),
            in_specs=[
                pl.BlockSpec((1, rows, width), lambda i, tab, ln: (tab[0], 0, 0)),
                pl.BlockSpec((1, rows, 2, kv_width), lambda i, tab, ln: (tab[0], 0, 0, 0)),
                pl.BlockSpec(memory_space=pltpu.HBM),
            ],
            out_specs=pl.BlockSpec((rows, width), lambda i, tab, ln: (0, 0)),
            scratch_shapes=[
                pltpu.VMEM((rows * (head_count + 8), HEAD_SIZE), F32),
                pltpu.VMEM((rows,) + cache.shape[1:], BF16),
                pltpu.SemaphoreType.DMA((rows // chunk,)),
            ],
        ),
        out_shape=jax.ShapeDtypeStruct((rows, width), BF16),
        compiler_params=pltpu.CompilerParams(
            dimension_semantics=("arbitrary",), vmem_limit_bytes=12 << 20
        ),
        name="attend",
    )(
        part.reshape(1),
        *in_hbm(
            lengths,
            query.reshape(parts, rows, width),
            latest.reshape(parts, rows, 2, kv_width),
            cache,
        ),
    )


def in_hbm(*arrays):
    return [pltpu.with_memory_space_constraint(a, pltpu.HBM) for a in arrays]


def on_chip(*arrays):
    return [pltpu.with_memory_space_constraint(a, pltpu.VMEM) for a in arrays]


def project_kernel(count, steps, add_count, tab_ref, *refs):
    pieces, w_ref = refs[:count], refs[count]
    adds = refs[count + 1 : count + 1 + add_count]
    rows, width = pieces[0].shape
    columns = w_ref.shape[1]
    if steps:
        out_ref, buf, sems = refs[-3:]
        deep = width // steps
        copies = [
            pltpu.make_async_copy(
                w_ref.at[pl.ds(k * deep, deep)], buf.at[pl.ds(k * deep, deep)], sems.at[k]
            )
            for k in range(steps)
        ]
        for copy in copies:
            copy.start()
    else:
        out_ref, buf = refs[-1], w_ref
    lhs = jnp.concatenate([p[...].astype(F32) for p in pieces], axis=0).astype(BF16)
    if steps:
        for copy in copies:
            copy.wait()
    result = jnp.dot(lhs, buf[...], preferred_element_type=F32)
    for i in range(count):
        block = tab_ref[i]
        value = result[i * rows : (i + 1) * rows]
        for a in adds:
            value = value + a[block][:, :columns].astype(F32)
        out_ref[block] = value.astype(BF16)


def project(table, pieces, w_out, adds, given, resident):
    rows, _ = pieces[0].shape
    count = len(pieces)
    steps = 0 if resident else 4
    vmem = pl.BlockSpec(memory_space=pltpu.VMEM)
    hbm = pl.BlockSpec(memory_space=pltpu.HBM)
    shapes = [jax.ShapeDtypeStruct((count, rows, w_out.shape[1]), BF16)]
    if not resident:
        shapes.append(pltpu.VMEM(w_out.shape, BF16))
    operands = adds if adds else [given]
    made = pl.pallas_call(
        functools.partial(project_kernel, count, steps, len(adds)),
        in_specs=[pl.BlockSpec(memory_space=pltpu.SMEM)]
        + [vmem] * count
        + [vmem if resident else hbm]
        + [vmem] * len(operands),
        out_specs=[vmem] * len(shapes),
        out_shape=shapes,
        scratch_shapes=[pltpu.SemaphoreType.DMA((steps,))] if steps else [],
        compiler_params=pltpu.CompilerParams(vmem_limit_bytes=16 << 20),
        name="project",
    )(table, *pieces, *(on_chip if resident else in_hbm)(w_out), *operands)
    return made[0], w_out if resident else made[1]


def down_product(acts, wd_buf, tab_ref, outs):
    local, hidden, features = wd_buf.shape
    chips = acts[0].shape[1]
    count = chips * CORES
    core = tab_ref[count + 1]
    aligned = hidden % 128 == 0
    left = []
    for e in range(local):
        picked = [
            act[e, tab_ref[count + 2 + s], half].astype(F32)
            for half in (1 - core, core)
            for act in acts
            for s in range(chips)
        ]
        left.append(jnp.concatenate(picked, axis=0).astype(BF16))
    if aligned:
        left = [jnp.concatenate(left, axis=1)]
    rows = left[0].shape[0] // 2
    wide = features * 2 // len(outs)
    block = min(wide, 1024)
    for first in range(0, features, block):
        source = slice(first, first + block)
        if aligned:
            right = [wd_buf[:, :, source].reshape(local * hidden, block)]
        else:
            right = [wd_buf[e, :, source] for e in range(local)]
        result = sum(jnp.dot(l, r, preferred_element_type=F32) for l, r in zip(left, right))
        result = result.astype(BF16)
        span = slice(first % wide, first % wide + block)
        for k in range(2):
            out_ref = outs[first // wide * 2 + k]
            value = result[k * rows : (k + 1) * rows].reshape(out_ref.shape[:3] + (block,))
            out_ref[:, :, :, span] = value


def up_kernel(jobs, acts_in, pieces, resident, count, tab_ref, *refs):
    refs = list(refs)
    take = lambda k: [refs.pop(0) for _ in range(k)]
    slices = [dict(zip(picked, take(len(picked)))) for _, picked, _, _ in jobs]
    starts = [take(2) if begun else None for _, _, begun, _ in jobs]
    gain_ref, weight_ref = take(2)
    acts = take(acts_in)
    wg_ref, wu_ref, wd_ref = take(3)
    results = [take(1 if ended else 2) for _, _, _, ended in jobs if not (ended and pieces)]
    own_ref = take(1)[0] if jobs[0][0] == 0 else None
    outs = take(2 * pieces)
    if resident:
        wg_buf, wu_buf, wd_buf = wg_ref, wu_ref, wd_ref
    else:
        wg_buf, wu_buf, wd_buf, sems = take(4)
    if pieces:
        results = [take(1)] + results
    local, features, hidden = wg_ref.shape
    _, rows, columns = next(iter(slices[0].values())).shape
    total = count * rows
    aligned = hidden % 128 == 0
    used = sorted(set(i for _, picked, _, _ in jobs for i in picked))

    def span_of(i):
        return pl.ds(pl.multiple_of(tab_ref[i] * columns, columns), columns)

    copies = {}
    if not resident:
        copies = {
            i: [
                pltpu.make_async_copy(
                    src.at[:, span_of(i), :], dst.at[:, span_of(i), :], sems.at[k, i]
                )
                for k, (src, dst) in enumerate(((wg_ref, wg_buf), (wu_ref, wu_buf)))
            ]
            for i in range(count)
        }
        down = pltpu.make_async_copy(wd_ref, wd_buf, sems.at[2, 0])
        for i in copies:
            for copy in copies[i]:
                copy.start()
        down.start()
    sums, squares = [], []
    for begun in starts:
        if begun is None:
            sums.append(None)
            squares.append(jnp.zeros((total, 1), F32))
        else:
            parts = [begun[0][k] for k in range(2 * local)]
            sums.append([jnp.concatenate(parts, axis=1)] if aligned else parts)
            squares.append(begun[1][...])
    for i in used:
        span = span_of(i)
        gain = gain_ref[:, span].astype(F32)
        left = {}
        for n, held in enumerate(slices):
            if i in held:
                x = held[i][...].astype(F32).reshape(total, columns)
                squares[n] = squares[n] + jnp.sum(x * x, axis=1, keepdims=True)
                left[n] = (x * gain).astype(BF16)
                if jobs[n][0] == 0:
                    own_ref[:, span] = held[i][tab_ref[count]]
        for copy in copies.get(i, ()):
            copy.wait()
        weights = [w[e, span, :] for w in (wg_buf, wu_buf) for e in range(local)]
        if aligned:
            weights = [jnp.concatenate(weights, axis=1)]
        both = jnp.concatenate(list(left.values()), axis=0) if len(left) > 1 else left[next(iter(left))]
        both = [jnp.dot(both, w, preferred_element_type=F32) for w in weights]
        for k, n in enumerate(left):
            more = [b[k * total : (k + 1) * total] for b in both]
            sums[n] = more if sums[n] is None else [a + b for a, b in zip(sums[n], more)]
    for n, (part, _, _, ended) in enumerate(jobs):
        final = sums[n]
        if aligned:
            final = [final[0][:, k * hidden : (k + 1) * hidden] for k in range(2 * local)]
        if not ended:
            for k in range(2 * local):
                results[n][0][k] = final[k]
            results[n][1][...] = squares[n]
            continue
        act_ref = results[n][0]
        scale = lax.rsqrt(squares[n] * (1.0 / features) + 1e-06)
        for e in range(local):
            gate = final[e] * scale
            up = final[local + e] * scale
            chosen = weight_ref[part, :, e : e + 1]
            value = gate / (1.0 + jnp.exp(-gate)) * up * chosen
            value = jnp.where(chosen != 0.0, value, 0.0).astype(BF16)
            for i in range(count):
                act_ref[e, i // CORES, i % CORES] = value[i * rows : (i + 1) * rows]
        acts.append(act_ref)
    if not resident:
        down.wait()
    if pieces:
        down_product(acts, wd_buf, tab_ref, outs)


def expert_up(table, jobs, held, begun, gain, weights, matrices, acts, pieces, resident):
    count = len(held[0])
    local, features, hidden = matrices[0].shape
    _, rows, _ = held[0][0].shape
    chips = count // CORES
    vmem = pl.BlockSpec(memory_space=pltpu.VMEM)
    hbm = pl.BlockSpec(memory_space=pltpu.HBM)
    inputs, shapes = [], []
    for part, picked, _, _ in jobs:
        inputs += [held[part][i] for i in picked]
    for _, _, has, _ in jobs:
        inputs += list(begun) if has else []
    inputs += [gain.reshape(1, -1), weights]
    for part, _, _, ended in jobs:
        if ended:
            act_shape = (local, chips, CORES, rows, hidden)
            if not pieces:
                shapes.append(jax.ShapeDtypeStruct(act_shape, BF16))
        else:
            shapes.append(jax.ShapeDtypeStruct((2 * local, count * rows, hidden), F32))
            shapes.append(jax.ShapeDtypeStruct((count * rows, 1), F32))
    if jobs[0][0] == 0:
        shapes.append(jax.ShapeDtypeStruct((rows, features), BF16))
    inputs += acts
    specs = [vmem] * len(inputs) + [vmem if resident else hbm] * 3
    inputs += (on_chip if resident else in_hbm)(*matrices)
    if pieces:
        parts = len(acts) + sum(ended for _, _, _, ended in jobs)
        shape = jax.ShapeDtypeStruct((parts, chips, rows, features // pieces), BF16)
        shapes += [shape] * (2 * pieces)
    scratch = []
    if not resident:
        shapes += [pltpu.VMEM(m.shape, BF16) for m in matrices]
        scratch.append(pltpu.SemaphoreType.DMA((3, count)))
    if pieces:
        scratch.append(pltpu.VMEM(act_shape, BF16))
    return pl.pallas_call(
        functools.partial(up_kernel, jobs, len(acts), pieces, resident, count),
        in_specs=[pl.BlockSpec(memory_space=pltpu.SMEM)] + specs,
        out_specs=[vmem] * len(shapes),
        out_shape=shapes,
        scratch_shapes=scratch,
        compiler_params=pltpu.CompilerParams(vmem_limit_bytes=20 << 20),
        name="expert_up",
    )(table, *inputs)


def add_kernel(split, *refs):
    left, right = refs[0], refs[1]
    for k, out_ref in enumerate(refs[2:]):
        if split is None:
            out_ref[...] = (left[...].astype(F32) + right[...].astype(F32)).astype(out_ref.dtype)
            continue
        at = (k,) if split == 0 else (slice(None), k)
        out_ref[...] = (left[at].astype(F32) + right[at].astype(F32)).astype(out_ref.dtype)


def add(left, right, split=None):
    vmem = pl.BlockSpec(memory_space=pltpu.VMEM)
    if split is None:
        shapes = [jax.ShapeDtypeStruct(left.shape, BF16)]
    else:
        shape = left.shape[:split] + left.shape[split + 1 :]
        shapes = [
            jax.ShapeDtypeStruct(shape, F32 if k == 0 else BF16) for k in range(left.shape[split])
        ]
    result = pl.pallas_call(
        functools.partial(add_kernel, split),
        in_specs=[vmem] * 2,
        out_specs=[vmem] * len(shapes),
        out_shape=shapes,
        compiler_params=pltpu.CompilerParams(vmem_limit_bytes=12 << 20),
        name="add",
    )(left, right)
    return result[0] if split is None else result


def per_device(
    query,
    latest_key_value,
    cache,
    lengths,
    w_out,
    residual_in,
    norm_gain,
    expert_ids,
    route_weights,
    w_gate,
    w_up,
    w_down,
):
    count = lax.axis_size("expert")
    tensors = lax.axis_size("tensor")
    chips = count // CORES
    me = lax.axis_index("expert")
    mine = lax.axis_index("tensor")
    core = me % CORES
    chip = me // CORES
    token_count = query.shape[0]
    rows = token_count // tensors
    columns = w_out.shape[1]
    local = w_gate.shape[0]

    behind = jnp.take(jnp.array(chip_table(chips, -1), jnp.int32), chip, axis=0)
    ahead = jnp.take(jnp.array(chip_table(chips, 1), jnp.int32), chip, axis=0)
    blocks = jnp.concatenate([behind * CORES + core, behind * CORES + (1 - core)])
    table = jnp.concatenate([blocks, me[None], core[None], ahead]).astype(jnp.int32)

    named = expert_ids[:, :, None] == jnp.arange(local * count, dtype=jnp.int32)
    dense = jnp.sum(jnp.where(named, route_weights[:, :, None], 0.0), axis=1)
    high = dense.astype(BF16)
    low = (dense - high.astype(F32)).astype(BF16)
    pair = jnp.stack([high, low], axis=-1).reshape(tensors, rows, count, local * 2)
    pair = jnp.roll(pair, -mine, axis=0)
    pair = pair.transpose(2, 1, 0, 3).reshape(count, rows, tensors * local * 2)
    pair = jnp.pad(pair, ((0, 0), (0, 0), (0, 128 - pair.shape[2])))
    shares = residual_in.reshape(rows, count, columns).transpose(1, 0, 2)
    packed = jnp.concatenate([shares, pair], axis=2)
    given = lax.all_to_all(packed, "expert", split_axis=0, concat_axis=0, tiled=True)
    pair = given[:, :, columns : columns + tensors * local * 2].astype(F32)
    pair = pair.reshape(count, rows, tensors, local, 2).sum(axis=-1)
    weights = pair.transpose(2, 0, 1, 3).reshape(tensors, count * rows, local)

    passed = []
    for j in range(1, tensors + 1):
        part = (mine + j) % tensors
        attended = attend(part, query, latest_key_value, cache, lengths, tensors)
        pieces = chip_gather(attended, chips)
        pieces = pieces + [core_swap(p, chips) for p in pieces]
        adds = [] if j < tensors else passed + [given]
        stream, w_out = project(table, pieces, w_out, adds, given, j > 1)
        if j < tensors:
            passed.append(tensor_shift(stream, tensors, -j))

    gathered = chip_gather(stream, chips)
    held = []
    for j in range(tensors):
        rows_of = gathered
        if j:
            rows_of = [tensor_shift(p, tensors, j) for p in gathered]
        held.append(rows_of + [core_swap(p, chips) for p in rows_of])

    everything = tuple(range(count))
    early = tuple(i for i in everything if i % chips < 2) if tensors > 1 else ()
    late = tuple(i for i in everything if i not in early)
    final = tensors - 1
    matrices = [w_gate, w_up, w_down]
    acts, begun = [], ()
    for j in range(tensors):
        jobs = [(j, late if early and j == final else everything, bool(early) and j == final, True)]
        if j == 0 and early:
            jobs.append((final, early, False, False))
        pieces = 2 if j == final else 0
        made = list(
            expert_up(
                table, jobs, held, begun, norm_gain, weights, matrices,
                acts if pieces else [], pieces, j > 0,
            )
        )
        if not pieces:
            acts.append(made.pop(0))
        if len(jobs) > 1:
            begun = (made.pop(0), made.pop(0))
        if j == 0:
            mine_rows = made.pop(0)
            matrices = made[2 * pieces :]

    swapped = [core_swap(made[2 * p], chips) for p in range(2)]
    sums = []
    for p, split in enumerate((1, 0)):
        first = add(made[2 * p + 1], swapped[p], split)
        if split == 1:
            total = first[0]
            for moved in chip_scatter(first, chips):
                total = total + moved.astype(F32)
            kept = total[0]
            for j in range(1, tensors):
                moved = tensor_shift(total[j].astype(BF16), tensors, -j)
                kept = kept + moved.astype(F32)
        else:
            kept = first[0]
            for j in range(1, tensors):
                moved = tensor_shift(first[j], tensors, -j)
                if j < tensors - 1:
                    kept = kept + moved.astype(F32)
            if tensors > 1:
                first = add(kept, moved, 0)
            else:
                first = [kept[0]] + [kept[s].astype(BF16) for s in range(1, chips)]
            kept = first[0]
            for moved in chip_scatter(first, chips):
                kept = kept + moved.astype(F32)
        sums.append(kept)
    return (mine_rows.astype(F32) + jnp.concatenate(sums, axis=1)).astype(BF16)


def solution(mesh):
    placed = (
        P(("groups", "expert"), "tensor"),
        P(("groups", "expert"), None, "tensor"),
        P(("groups", "expert"), None, None, "tensor"),
        P(("groups", "expert")),
        P("tensor", "expert"),
        P(("groups", "expert", "tensor"), None),
        P(),
        P(("groups", "expert"), None),
        P(("groups", "expert"), None),
        P("expert", None, "tensor"),
        P("expert", None, "tensor"),
        P("expert", "tensor", None),
    )

    return jax.shard_map(
        per_device,
        mesh=mesh,
        in_specs=placed,
        out_specs=P(("groups", "expert", "tensor"), None),
        check_vma=False,
    )
```
